512 devices in a mesh: groups: 2 (over y), dp: 16 (over z), head: 8 (over x), sub: 2 (over core).
Axes of the slice: x: 8, y: 2, z: 16, core: 2. Of those that a mesh axis runs over, the one named last changes fastest.
The devices are a block of a 8x8x16 slice.
Arguments:
- queries: bfloat16 [512, 64, 128], P(('groups', 'dp', 'sub'), 'head'), parts along dimension 0, may hold values from -8 to 8
- kv_cache: bfloat16 [32768, 8, 2, 16, 128], P(('groups', 'dp', 'sub'), 'head'), parts along dimension 0, may hold values from -8 to 8
- keep: int32 [512, 48], P(('groups', 'dp', 'sub')), parts along dimension 0, may hold values from 0 to 63, as said below
- lengths: int32 [512], P(('groups', 'dp', 'sub')), parts along dimension 0, may hold values from 384 to 768
- placement: int32 [512, 64], P(('groups', 'dp', 'sub')), parts along dimension 0, may hold values from 0 to 16383, as said below
- positions: int32 [512], P(('groups', 'dp', 'sub')), parts along dimension 0, may hold values from 0 to 4095
Outputs:
- attention: bfloat16 [512, 64, 128], P(('groups', 'dp', 'sub'), 'head'), parts along dimension 0
- log_norm: float32 [512, 64], P(('groups', 'dp', 'sub'), 'head'), parts along dimension 0
The draws below stay inside these ranges and needn't reach their ends.
There are 2 independent parts, one for each index of `groups`. The reference program is written for one: setup_inputs(seed, part) draws one part's arguments, and reference() takes and returns one part's arrays. A program takes and returns all parts, laid end to end along the dimension named above; each array names one. Nothing has to cross between parts.
Inputs may be any that keep to these rules, and one draw needn't show every extreme that they name: `keep`: each row holds distinct block numbers in increasing order. `placement`: every cache row is named once; the 8 requests of one device (aligned groups of 8 rows) have exactly 16 of their blocks in the cache rows of each device.
All inputs are finite; a program needn't handle non-finite values.
Results may differ from the reference program's by a relative error of at most 0.0058.
Values may be sent and summed in bfloat16 or wider, within the bound.
No kernel may reach another device: no remote copies, remote signals or barrier semaphores. Data moves between devices by JAX's collectives and lax.ppermute only.
A program may use at most 64 MiB of HBM per device.

```python
import jax
import jax.numpy as jnp
from jax import lax

QH = 64
KVH = 8
HD = 128
BLK = 16
NBR = 64
KEEP = 48
OWNERS = 32
REQ = 256
POOL = 16384
SPREAD = 16


def draw_queries(key, part):
    first = jax.random.fold_in(key, 1)
    values = jnp.clip(jax.random.normal(first, (REQ, QH, HD), jnp.float32), -4.0, 4.0)
    return values.astype(jnp.bfloat16)


def draw_kv_cache(key, part):
    first = jax.random.fold_in(key, 2)
    second = jax.random.fold_in(key, 4)
    keys = jnp.clip(1.5 * jax.random.normal(first, (POOL, KVH, BLK, HD), jnp.float32), -6.0, 6.0)
    values = jnp.clip(jax.random.normal(second, (POOL, KVH, BLK, HD), jnp.float32), -4.0, 4.0)
    return jnp.stack([keys, values], axis=2).astype(jnp.bfloat16)


def draw_keep(key, part):
    row_keys = jax.random.split(jax.random.fold_in(key, 3), REQ)
    rows = jax.vmap(lambda one: jnp.sort(jax.random.permutation(one, NBR)[:KEEP]))(row_keys)
    return rows.astype(jnp.int32)


def draw_placement(key, part):
    pool_dev = OWNERS * SPREAD
    owner_keys = jax.random.split(jax.random.fold_in(key, 5), OWNERS)
    slot_order = jax.vmap(lambda one: jax.random.permutation(one, pool_dev))(owner_keys).astype(jnp.int32)
    offsets = (jnp.arange(OWNERS, dtype=jnp.int32) * pool_dev)[:, None, None]
    physical = (slot_order.reshape(OWNERS, OWNERS, SPREAD) + offsets).transpose(1, 0, 2).reshape(OWNERS, pool_dev)
    device_keys = jax.random.split(jax.random.fold_in(key, 7), OWNERS)
    order = jax.vmap(lambda one: jax.random.permutation(one, pool_dev))(device_keys).astype(jnp.int32)
    table = jax.vmap(lambda where_to, what: jnp.zeros((pool_dev,), jnp.int32).at[where_to].set(what))(order, physical)
    return table.reshape(REQ, NBR).astype(jnp.int32)


def place_ends(values, stream_key, low, top_value):
    index_at = [jax.random.randint(jax.random.fold_in(stream_key, axis), (), 0, length) for axis, length in enumerate(values.shape)]
    widest = values.shape.index(max(values.shape))
    next_to = index_at[:widest] + [(index_at[widest] + 1) % values.shape[widest]] + index_at[widest + 1:]
    return values.at[tuple(index_at)].set(low).at[tuple(next_to)].set(top_value)


def setup_inputs(seed: int = 0, part: int = 0) -> dict:
    arg_keys = jax.random.split(jax.random.key(seed), 7)
    part_splits = jax.random.split(jax.random.fold_in(arg_keys[6], part), 7)
    queries = draw_queries(jax.random.fold_in(jax.random.fold_in(arg_keys[6], part), 71), part)
    kv_cache = draw_kv_cache(jax.random.fold_in(jax.random.fold_in(arg_keys[6], part), 71), part)
    keep = draw_keep(jax.random.fold_in(jax.random.fold_in(arg_keys[6], part), 71), part)
    lengths = place_ends(jax.random.randint(part_splits[3], (REQ,), KEEP * BLK // 2, KEEP * BLK + 1), jax.random.fold_in(part_splits[3], 1), KEEP * BLK // 2, KEEP * BLK).astype(jnp.int32)
    placement = draw_placement(jax.random.fold_in(jax.random.fold_in(arg_keys[6], part), 71), part)
    positions = place_ends(jax.random.randint(part_splits[5], (REQ,), 0, 4096), jax.random.fold_in(part_splits[5], 1), 0, 4095).astype(jnp.int32)
    return dict(queries=queries, kv_cache=kv_cache, keep=keep, lengths=lengths, placement=placement, positions=positions)


def rotate(values, positions):
    half = values.shape[-1] // 2
    inverse = 1000000.0 ** (-(2.0 * jnp.arange(half, dtype=jnp.float32)) / values.shape[-1])
    angle = positions.astype(jnp.float32)[:, None] * inverse[None, :]
    cosine = jnp.cos(angle)[:, None, :]
    sine = jnp.sin(angle)[:, None, :]
    first = values[..., :half]
    second = values[..., half:]
    return jnp.concatenate([first * cosine - second * sine, second * cosine + first * sine], axis=-1)


def reference(queries, kv_cache, keep, lengths, placement, positions):
    group = QH // KVH
    factor = HD ** -0.5
    rotated = rotate(queries.astype(jnp.float32), positions).astype(jnp.bfloat16)

    def single(items):
        query, kept, length, table = items
        rows = jnp.take(table, kept).astype(jnp.int32)
        blocks = jnp.take(kv_cache, rows, axis=0)
        keys = blocks[:, :, 0].astype(jnp.float32)
        values = blocks[:, :, 1].astype(jnp.float32)
        grouped = query.reshape(KVH, group, HD).astype(jnp.float32)
        scores = jnp.einsum("kgd,bktd->bkgt", grouped, keys) * factor
        tokens = jnp.arange(KEEP, dtype=jnp.int32)[:, None] * BLK + jnp.arange(BLK, dtype=jnp.int32)[None, :]
        live = (tokens < length)[:, None, None, :]
        peak = jnp.max(jnp.where(live, scores, -1e30), axis=-1)
        weights = jnp.where(live, jnp.exp(scores - peak[..., None]), 0.0).astype(jnp.bfloat16)
        totals = jnp.sum(weights.astype(jnp.float32), axis=-1)
        partial_value = jnp.einsum("bkgt,bktd->bkgd", weights.astype(jnp.float32), values)
        top = jnp.max(peak, axis=0)
        scale = jnp.exp(peak - top[None])
        norm = jnp.sum(scale * totals, axis=0)
        merged = jnp.einsum("bkg,bkgd->kgd", scale, partial_value, precision=lax.Precision.HIGHEST)
        output = (merged / norm[..., None]).reshape(QH, HD).astype(jnp.bfloat16)
        return output, (top + jnp.log(norm)).reshape(QH)

    attention, log_norm = lax.map(single, (rotated, keep, lengths, placement))
    return attention, log_norm
```

```python
import jax
import jax.numpy as jnp
from jax import lax
from jax.experimental import pallas as pl
from jax.experimental.pallas import tpu as pltpu
from jax.sharding import PartitionSpec as P

LANES = 128
LOW = -1e30


def iota(shape, dim):
    return lax.broadcasted_iota(jnp.int32, shape, dim)


def bits(n):
    assert n & (n - 1) == 0
    return n.bit_length() - 1


def angles(positions, head_dim):
    half = head_dim // 2
    inverse = 1000000.0 ** (-(2.0 * jnp.arange(half, dtype=jnp.float32)) / head_dim)
    angle = positions.astype(jnp.float32)[:, None] * inverse[None, :]
    cosine, sine = jnp.cos(angle), jnp.sin(angle)
    return jnp.concatenate([cosine, cosine], axis=1), jnp.concatenate([-sine, sine], axis=1)


def pack(queries, cosine, sine, keep, lengths, placement, chips, cores, pool_dev, block_len):
    requests, heads, head_dim = queries.shape
    kept, blocks = keep.shape[1], placement.shape[1]
    owners = chips * cores
    spread = requests * blocks // owners
    rows = requests * heads
    parts = requests * blocks // LANES
    per = requests // parts
    assert per * blocks == LANES and 4 * cores * spread == LANES and head_dim == LANES
    pool_bits, owner_bits, len_bits, req_bits = bits(pool_dev), bits(cores), bits(block_len), bits(requests)

    def body(lengths_ref, q_ref, cos_ref, sin_ref, keep_ref, place_ref, out_ref):
        place = place_ref[...]
        kept_ids = keep_ref[...]
        req = iota((requests, blocks), 0)
        lane = iota((requests, blocks), 1)
        length = jnp.zeros((requests, blocks), jnp.int32)
        for r in range(requests):
            length = jnp.where(req == r, lengths_ref[r], length)
        count = jnp.zeros((requests, blocks), jnp.int32)
        for s in range(kept):
            count = jnp.where(kept_ids[:, s : s + 1] == lane, jnp.clip(length - s * block_len, 0, block_len), count)
        owner = place >> pool_bits
        owner = (owner & (cores - 1)) * chips + (owner >> owner_bits)
        word = (place & (pool_dev - 1)) | (req << pool_bits) | (count << (pool_bits + req_bits))
        owner = jnp.concatenate([owner[p * parts : (p + 1) * parts] for p in range(per)], axis=1)
        word = jnp.concatenate([word[p * parts : (p + 1) * parts] for p in range(per)], axis=1).astype(jnp.float32)
        mine = iota((owners, LANES), 0)
        hits = [owner[j : j + 1] == mine for j in range(parts)]
        ones = jnp.concatenate([jnp.where(h, 1.0, 0.0) for h in hits], axis=0).astype(jnp.bfloat16)
        before = jnp.where(iota((LANES, LANES), 0) < iota((LANES, LANES), 1), 1.0, 0.0).astype(jnp.bfloat16)
        within = jnp.dot(ones, before, preferred_element_type=jnp.float32)
        totals = jnp.dot(ones, jnp.ones((LANES, LANES), jnp.bfloat16), preferred_element_type=jnp.float32)
        ranks, start = [], jnp.zeros((owners, LANES), jnp.float32)
        for j in range(parts):
            ranks.append(jnp.where(hits[j], within[j * owners : (j + 1) * owners] + start, -1.0))
            start = start + totals[j * owners : (j + 1) * owners]
        col = iota((owners, LANES), 1)
        table = jnp.zeros((owners, LANES), jnp.float32)
        for k in range(spread):
            found = jnp.zeros((owners, LANES), jnp.float32)
            for j in range(parts):
                found = jnp.where(ranks[j] == k, word[j : j + 1], found)
            table = jnp.where((col & (spread - 1)) == k, jnp.sum(found, axis=1, keepdims=True), table)
        table = table.astype(jnp.int32)
        lane = iota((chips, LANES), 1)
        slots = table[:chips]
        for c in range(1, cores):
            slots = jnp.where(((lane >> bits(spread)) & (cores - 1)) == c, table[c * chips : (c + 1) * chips], slots)
        field = lane >> bits(spread * cores)
        low_bits = bits(block_len)
        row_hi = (slots & (pool_dev - 1)) >> low_bits
        row_lo = slots & (block_len - 1)
        of_req = (slots >> pool_bits) & (requests - 1)
        live = slots >> (pool_bits + req_bits)
        meta = jnp.where(field == 0, row_hi, jnp.where(field == 1, row_lo, jnp.where(field == 2, of_req, live)))
        meta = meta.astype(jnp.float32)
        turned = []
        for r in range(requests):
            x = q_ref[r].astype(jnp.float32)
            turned.append(x * cos_ref[r : r + 1] + pltpu.roll(x, head_dim // 2, 1) * sin_ref[r : r + 1])
        turned = jnp.concatenate(turned, axis=0).astype(jnp.bfloat16)
        sub = iota((8, LANES), 0)
        for d in range(chips):
            out_ref[d, :rows, :] = turned
            out_ref[d, rows:, :] = jnp.where(sub == 0, meta[d : d + 1], 0.0).astype(jnp.bfloat16)

    vmem = pl.BlockSpec(memory_space=pltpu.VMEM)
    return pl.pallas_call(
        body,
        name="pack",
        out_shape=jax.ShapeDtypeStruct((chips, rows + 8, LANES), jnp.bfloat16),
        in_specs=[pl.BlockSpec(memory_space=pltpu.SMEM)] + [vmem] * 5,
        out_specs=vmem,
    )(lengths, queries, cosine, sine, keep, placement)


def attend(core, kv, got, requests, block_len):
    cores, chips, height, _ = got.shape
    rows = height - 8
    heads = rows // requests
    sources = cores * chips
    spread = LANES // (4 * cores)
    tokens = spread * block_len
    factor = LANES ** (-0.5)
    height_out = chips * rows + rows

    def body(core_ref, kv_ref, got_ref, out_ref, ids_ref, live_ref, rows_ref, sem):
        at = core_ref[0] * spread
        meta = jnp.concatenate(
            [got_ref[c, z, rows:, :].astype(jnp.float32)[:1] for c in range(cores) for z in range(chips)], axis=0
        ).astype(jnp.bfloat16)
        wide = cores * spread
        src, dst = iota((LANES, LANES), 0), iota((LANES, LANES), 1)
        inside = dst < spread
        pick = jnp.where(inside & (src == at + dst), float(block_len), 0.0) + jnp.where(inside & (src == wide + at + dst), 1.0, 0.0)
        ids = jnp.dot(meta, pick.astype(jnp.bfloat16), preferred_element_type=jnp.float32)
        ids_ref[...] = ids.astype(jnp.int32)
        copy = pltpu.make_async_copy(ids_ref, rows_ref, sem)
        copy.start()
        src, dst = iota((LANES, tokens), 0), iota((LANES, tokens), 1) >> bits(block_len)
        pick_req = jnp.where(src == 2 * wide + at + dst, 1.0, 0.0).astype(jnp.bfloat16)
        pick_live = jnp.where(src == 3 * wide + at + dst, 1.0, 0.0).astype(jnp.bfloat16)
        of_req = jnp.dot(meta, pick_req, preferred_element_type=jnp.float32)
        count = jnp.dot(meta, pick_live, preferred_element_type=jnp.float32)
        step = (iota((sources, tokens), 1) & (block_len - 1)).astype(jnp.float32)
        live_ref[...] = jnp.where(step < count, of_req, -1.0)
        copy.wait()
        request = (iota((rows, tokens), 0) >> bits(heads)).astype(jnp.float32)
        lane = iota((rows, LANES), 1)
        fill = jnp.ones((tokens, LANES), jnp.bfloat16)

        for c in range(cores):

            def one(z, stats, c=c):
                s = c * chips + z
                q = got_ref[c, z, :rows, :]
                ks, vs = [], []
                for k in range(spread):
                    row = rows_ref[s, k]
                    ks.append(kv_ref[row, :block_len, :])
                    vs.append(kv_ref[row, block_len:, :])
                ks = jnp.concatenate(ks, axis=0)
                vs = jnp.concatenate([jnp.concatenate(vs, axis=0), fill], axis=1)
                score = lax.dot_general(q, ks, (((1,), (1,)), ((), ())), preferred_element_type=jnp.float32) * factor
                mine = live_ref[pl.ds(s, 1), :] == request
                score = jnp.where(mine, score, LOW)
                peak = jnp.max(score, axis=1, keepdims=True)
                weight = jnp.where(mine, jnp.exp(score - peak), 0.0).astype(jnp.bfloat16)
                both = jnp.dot(weight, vs, preferred_element_type=jnp.float32)
                total = both[:, LANES:]
                some = total > 0.0
                safe = jnp.where(some, total, 1.0)
                out_ref[c, pl.ds(pl.multiple_of(z * rows, rows), rows), :] = both[:, :LANES] / safe
                return jnp.where(lane == z, jnp.where(some, peak + jnp.log(safe), LOW), stats)

            stats = lax.fori_loop(0, chips, one, jnp.full((rows, LANES), LOW, jnp.float32), unroll=2)
            out_ref[c, chips * rows :, :] = stats

    vmem = pl.BlockSpec(memory_space=pltpu.VMEM)
    return pl.pallas_call(
        body,
        name="attend",
        out_shape=jax.ShapeDtypeStruct((cores, height_out, LANES), jnp.float32),
        in_specs=[pl.BlockSpec(memory_space=pltpu.SMEM), vmem, vmem],
        out_specs=vmem,
        scratch_shapes=[
            pltpu.VMEM((sources, LANES), jnp.int32),
            pltpu.VMEM((sources, tokens), jnp.float32),
            pltpu.SMEM((sources, LANES), jnp.int32),
            pltpu.SemaphoreType.DMA,
        ],
    )(core, kv, got)


def square(x):
    return jnp.concatenate([x, jnp.zeros((LANES - x.shape[0], LANES), x.dtype)], axis=0).T


def merge_pair(halves, chips):
    cores, height, _ = halves.shape
    rows = height // (chips + 1)

    def body(x_ref, out_ref):
        logs = [x_ref[c, chips * rows :, :] for c in range(cores)]
        top = logs[0]
        for one in logs[1:]:
            top = jnp.maximum(top, one)
        scale = [jnp.exp(one - top) for one in logs]
        norm = sum(scale[1:], scale[0])
        weight = [one / norm for one in scale]
        whole = square(top + jnp.log(norm))[:chips]
        first = whole.astype(jnp.bfloat16).astype(jnp.float32)
        rest = whole - first
        second = rest.astype(jnp.bfloat16).astype(jnp.float32)
        third = rest - second
        sub = iota((8, LANES), 0)
        for d in range(chips):
            mixed = sum(weight[c][:, d : d + 1] * x_ref[c, d * rows : (d + 1) * rows, :] for c in range(cores))
            out_ref[d, :rows, :] = mixed.astype(jnp.bfloat16)
            tail = jnp.where(sub == 0, first[d : d + 1], jnp.where(sub == 1, second[d : d + 1], third[d : d + 1]))
            out_ref[d, rows:, :] = tail.astype(jnp.bfloat16)

    vmem = pl.BlockSpec(memory_space=pltpu.VMEM)
    return pl.pallas_call(
        body,
        name="merge_pair",
        out_shape=jax.ShapeDtypeStruct((chips, rows + 8, LANES), jnp.bfloat16),
        in_specs=[vmem],
        out_specs=vmem,
    )(halves)


def finish(got, requests):
    chips, height, _ = got.shape
    rows = height - 8
    heads = rows // requests

    def body(x_ref, att_ref, log_ref):
        logs = []
        for s in range(chips):
            tail = x_ref[s, rows:, :].astype(jnp.float32)
            logs.append(tail[0:1] + tail[1:2] + tail[2:3])
        logs = jnp.concatenate(logs, axis=0)
        top = jnp.max(logs, axis=0, keepdims=True)
        scale = jnp.exp(logs - top)
        norm = jnp.sum(scale, axis=0, keepdims=True)
        log_norm = jnp.broadcast_to(top + jnp.log(norm), (requests, LANES))
        weight = square(scale / norm)[:rows]
        merged = sum(weight[:, s : s + 1] * x_ref[s, :rows, :].astype(jnp.float32) for s in range(chips))
        att_ref[...] = merged.reshape(requests, heads, LANES).astype(jnp.bfloat16)
        sub = iota((requests, LANES), 0)
        spread = log_norm
        for r in range(1, requests):
            spread = jnp.where(sub == r, pltpu.roll(log_norm, LANES - r * heads, 1), spread)
        log_ref[...] = spread[:, :heads]

    vmem = pl.BlockSpec(memory_space=pltpu.VMEM)
    return pl.pallas_call(
        body,
        name="finish",
        out_shape=(
            jax.ShapeDtypeStruct((requests, heads, LANES), jnp.bfloat16),
            jax.ShapeDtypeStruct((requests, heads), jnp.float32),
        ),
        in_specs=[vmem],
        out_specs=(vmem, vmem),
    )(got)


def local(queries, kv_cache, keep, lengths, placement, positions):
    chips, cores = lax.axis_size("dp"), lax.axis_size("sub")
    requests, q_heads, head_dim = queries.shape
    pool_dev, kv_heads, _, block_len, _ = kv_cache.shape
    assert kv_heads == 1
    cosine, sine = angles(positions, head_dim)
    message = pack(queries, cosine, sine, keep, lengths, placement, chips, cores, pool_dev, block_len)
    asked = lax.all_to_all(message, "dp", 0, 0, tiled=True)
    asked = lax.all_gather(asked, "sub")
    core = lax.axis_index("sub").reshape(1).astype(jnp.int32)
    partials = attend(core, kv_cache.reshape(pool_dev, 2 * block_len, head_dim), asked, requests, block_len)
    halves = lax.all_to_all(partials, "sub", 0, 0, tiled=True)
    answer = lax.all_to_all(merge_pair(halves, chips), "dp", 0, 0, tiled=True)
    return finish(answer, requests)


def solution(mesh):
    in_specs = (
        P(("groups", "dp", "sub"), "head", None),
        P(("groups", "dp", "sub"), "head", None, None, None),
        P(("groups", "dp", "sub"), None),
        P(("groups", "dp", "sub")),
        P(("groups", "dp", "sub"), None),
        P(("groups", "dp", "sub")),
    )
    out_specs = (P(("groups", "dp", "sub"), "head", None), P(("groups", "dp", "sub"), "head"))
    return jax.shard_map(local, mesh=mesh, in_specs=in_specs, out_specs=out_specs, check_vma=False)
```

```python
import jax
import jax.numpy as jnp
import numpy as np
from jax import lax
from jax.experimental import pallas as pl
from jax.experimental.pallas import tpu as pltpu
from jax.sharding import PartitionSpec as P

LANES = 128
LOW = -1e30
UNROLL = 4
PACK_LIMIT = 60 * 1024
ATTEND_LIMIT = 52000


def iota(shape, dim):
    return lax.broadcasted_iota(jnp.int32, shape, dim)


def bits(n):
    assert n & (n - 1) == 0
    return n.bit_length() - 1


def frequencies(head_dim, rows):
    half = head_dim // 2
    inverse = 1000000.0 ** (-(2.0 * np.arange(half)) / head_dim)
    return jnp.asarray(np.tile(inverse, (rows, head_dim // half)), jnp.float32)


def limit(kib):
    return pltpu.CompilerParams(vmem_limit_bytes=kib << 10)


def pack(queries, positions, keep, lengths, placement, chips, cores, pool_dev, block_len):
    requests, heads, head_dim = queries.shape
    kept, blocks = keep.shape[1], placement.shape[1]
    owners = chips * cores
    spread = requests * blocks // owners
    rows = requests * heads
    parts = requests * blocks // LANES
    per = requests // parts
    assert per * blocks == LANES and 4 * cores * spread == LANES and head_dim == LANES
    pool_bits, owner_bits, len_bits, req_bits = bits(pool_dev), bits(cores), bits(block_len), bits(requests)

    def body(lengths_ref, positions_ref, q_ref, freq_ref, keep_ref, place_ref, out_ref):
        place = place_ref[...]
        kept_ids = keep_ref[...]
        req = iota((requests, blocks), 0)
        lane = iota((requests, blocks), 1)
        length = jnp.zeros((requests, blocks), jnp.int32)
        for r in range(requests):
            length = jnp.where(req == r, lengths_ref[r], length)
        count = jnp.zeros((requests, blocks), jnp.int32)
        for s in range(kept):
            count = jnp.where(kept_ids[:, s : s + 1] == lane, jnp.clip(length - s * block_len, 0, block_len), count)
        owner = place >> pool_bits
        owner = (owner & (cores - 1)) * chips + (owner >> owner_bits)
        word = (place & (pool_dev - 1)) | (req << pool_bits) | (count << (pool_bits + req_bits))
        owner = jnp.concatenate([owner[p * parts : (p + 1) * parts] for p in range(per)], axis=1)
        word = jnp.concatenate([word[p * parts : (p + 1) * parts] for p in range(per)], axis=1).astype(jnp.float32)
        mine = iota((owners, LANES), 0)
        hits = [owner[j : j + 1] == mine for j in range(parts)]
        ones = jnp.concatenate([jnp.where(h, 1.0, 0.0) for h in hits], axis=0).astype(jnp.bfloat16)
        before = jnp.where(iota((LANES, LANES), 0) < iota((LANES, LANES), 1), 1.0, 0.0).astype(jnp.bfloat16)
        within = jnp.dot(ones, before, preferred_element_type=jnp.float32)
        totals = jnp.dot(ones, jnp.ones((LANES, LANES), jnp.bfloat16), preferred_element_type=jnp.float32)
        ranks, start = [], jnp.zeros((owners, LANES), jnp.float32)
        for j in range(parts):
            ranks.append(jnp.where(hits[j], within[j * owners : (j + 1) * owners] + start, -1.0))
            start = start + totals[j * owners : (j + 1) * owners]
        col = iota((owners, LANES), 1)
        table = jnp.zeros((owners, LANES), jnp.float32)
        for k in range(spread):
            found = jnp.zeros((owners, LANES), jnp.float32)
            for j in range(parts):
                found = jnp.where(ranks[j] == k, word[j : j + 1], found)
            table = jnp.where((col & (spread - 1)) == k, jnp.sum(found, axis=1, keepdims=True), table)
        table = table.astype(jnp.int32)
        lane = iota((chips, LANES), 1)
        slots = table[:chips]
        for c in range(1, cores):
            slots = jnp.where(((lane >> bits(spread)) & (cores - 1)) == c, table[c * chips : (c + 1) * chips], slots)
        field = lane >> bits(spread * cores)
        low_bits = bits(block_len)
        row_hi = (slots & (pool_dev - 1)) >> low_bits
        row_lo = slots & (block_len - 1)
        of_req = (slots >> pool_bits) & (requests - 1)
        live = slots >> (pool_bits + req_bits)
        meta = jnp.where(field == 0, row_hi, jnp.where(field == 1, row_lo, jnp.where(field == 2, of_req, live)))
        meta = meta.astype(jnp.float32)
        row = iota((requests, head_dim), 0)
        position = jnp.zeros((requests, head_dim), jnp.int32)
        for r in range(requests):
            position = jnp.where(row == r, positions_ref[r], position)
        angle = position.astype(jnp.float32) * freq_ref[...]
        cosine, sine = jnp.cos(angle), jnp.sin(angle)
        sine = jnp.where(iota((requests, head_dim), 1) < head_dim // 2, -sine, sine)
        turned = []
        for r in range(requests):
            x = q_ref[r].astype(jnp.float32)
            turned.append(x * cosine[r : r + 1] + pltpu.roll(x, head_dim // 2, 1) * sine[r : r + 1])
        turned = jnp.concatenate(turned, axis=0).astype(jnp.bfloat16)
        sub = iota((8, LANES), 0)
        for d in range(chips):
            out_ref[d, :rows, :] = turned
            out_ref[d, rows:, :] = jnp.where(sub == 0, meta[d : d + 1], 0.0).astype(jnp.bfloat16)

    vmem = pl.BlockSpec(memory_space=pltpu.VMEM)
    return pl.pallas_call(
        body,
        name="pack",
        out_shape=jax.ShapeDtypeStruct((chips, rows + 8, LANES), jnp.bfloat16),
        in_specs=[pl.BlockSpec(memory_space=pltpu.SMEM)] * 2 + [vmem] * 4,
        out_specs=vmem,
        compiler_params=limit(PACK_LIMIT),
    )(lengths, positions, queries, frequencies(head_dim, requests), keep, placement)


def pieces(x):
    first = x.astype(jnp.bfloat16).astype(jnp.float32)
    rest = x - first
    second = rest.astype(jnp.bfloat16).astype(jnp.float32)
    return first, second, rest - second


def attend(kv, got, requests):
    cores, chips, height, _ = got.shape
    pool_dev, _, block_len, _ = kv.shape
    rows = height - 8
    heads = rows // requests
    sources = cores * chips
    spread = LANES // (4 * cores)
    tokens = spread * block_len
    factor = LANES ** (-0.5)

    def body(kv_ref, got_ref, out_ref, k_ref, v_ref, ids_ref, live_ref, weight_ref, rows_ref, sems):
        k_copy = pltpu.make_async_copy(kv_ref.at[:, 0], k_ref, sems.at[0])
        v_copy = pltpu.make_async_copy(kv_ref.at[:, 1], v_ref, sems.at[1])
        k_copy.start()
        v_copy.start()
        at = lax.axis_index("sub") * spread
        meta = jnp.concatenate(
            [got_ref[c, z, rows:, :].astype(jnp.float32)[:1] for c in range(cores) for z in range(chips)], axis=0
        ).astype(jnp.bfloat16)
        wide = cores * spread
        src, dst = iota((LANES, LANES), 0), iota((LANES, LANES), 1)
        inside = dst < spread
        pick = jnp.where(inside & (src == at + dst), float(block_len), 0.0) + jnp.where(inside & (src == wide + at + dst), 1.0, 0.0)
        ids = jnp.dot(meta, pick.astype(jnp.bfloat16), preferred_element_type=jnp.float32)
        ids_ref[...] = ids.astype(jnp.int32)
        copy = pltpu.make_async_copy(ids_ref, rows_ref, sems.at[2])
        copy.start()
        src, dst = iota((LANES, tokens), 0), iota((LANES, tokens), 1) >> bits(block_len)
        pick_req = jnp.where(src == 2 * wide + at + dst, 1.0, 0.0).astype(jnp.bfloat16)
        pick_live = jnp.where(src == 3 * wide + at + dst, 1.0, 0.0).astype(jnp.bfloat16)
        of_req = jnp.dot(meta, pick_req, preferred_element_type=jnp.float32)
        count = jnp.dot(meta, pick_live, preferred_element_type=jnp.float32)
        step = (iota((sources, tokens), 1) & (block_len - 1)).astype(jnp.float32)
        live_ref[...] = jnp.where(step < count, of_req, -1.0)
        request = (iota((rows, tokens), 0) >> bits(heads)).astype(jnp.float32)
        lane = iota((rows, LANES), 1)
        fill = jnp.ones((tokens, LANES), jnp.bfloat16)
        low = jnp.full((rows, LANES), LOW, jnp.float32)
        copy.wait()
        k_copy.wait()

        def held(ref, s):
            return jnp.concatenate([ref[rows_ref[s, k]] for k in range(spread)], axis=0)

        peaks = []
        for c in range(cores):

            def look(z, peak_of, c=c):
                s = c * chips + z
                score = (
                    lax.dot_general(
                        got_ref[c, z, :rows, :], held(k_ref, s), (((1,), (1,)), ((), ())), preferred_element_type=jnp.float32
                    )
                    * factor
                )
                mine = live_ref[pl.ds(s, 1), :] == request
                score = jnp.where(mine, score, LOW)
                peak = jnp.max(score, axis=1, keepdims=True)
                weight_ref[s] = jnp.where(mine, jnp.exp(score - peak), 0.0).astype(jnp.bfloat16)
                return jnp.where(lane == z, peak, peak_of)

            peaks.append(lax.fori_loop(0, chips, look, low, unroll=UNROLL))
        v_copy.wait()
        for c in range(cores):

            def add(z, total_of, c=c):
                s = c * chips + z
                vs = jnp.concatenate([held(v_ref, s), fill], axis=1)
                both = jnp.dot(weight_ref[s], vs, preferred_element_type=jnp.float32)
                total = both[:, LANES:]
                safe = jnp.where(total > 0.0, total, 1.0)
                out_ref[c, pl.ds(pl.multiple_of(z * rows, rows), rows), :] = (both[:, :LANES] / safe).astype(jnp.bfloat16)
                return jnp.where(lane == z, total, total_of)

            total = lax.fori_loop(0, chips, add, jnp.zeros((rows, LANES), jnp.float32), unroll=UNROLL)
            some = total > 0.0
            first, second, third = pieces(jnp.where(some, peaks[c] + jnp.log(jnp.where(some, total, 1.0)), LOW))
            second, third = pltpu.roll(second, chips, 1), pltpu.roll(third, 2 * chips, 1)
            out_ref[c, chips * rows :, :] = jnp.where(
                lane < chips, first, jnp.where(lane < 2 * chips, second, third)
            ).astype(jnp.bfloat16)

    vmem = pl.BlockSpec(memory_space=pltpu.VMEM)
    return pl.pallas_call(
        body,
        name="attend",
        out_shape=jax.ShapeDtypeStruct((cores, chips * rows + rows, LANES), jnp.bfloat16),
        in_specs=[pl.BlockSpec(memory_space=pltpu.HBM), vmem],
        out_specs=vmem,
        compiler_params=limit(ATTEND_LIMIT),
        scratch_shapes=[
            pltpu.VMEM((pool_dev, block_len, LANES), jnp.bfloat16),
            pltpu.VMEM((pool_dev, block_len, LANES), jnp.bfloat16),
            pltpu.VMEM((sources, LANES), jnp.int32),
            pltpu.VMEM((sources, tokens), jnp.float32),
            pltpu.VMEM((sources, rows, tokens), jnp.bfloat16),
            pltpu.SMEM((sources, LANES), jnp.int32),
            pltpu.SemaphoreType.DMA((3,)),
        ],
    )(kv, got)


def square(x):
    return jnp.concatenate([x, jnp.zeros((LANES - x.shape[0], LANES), x.dtype)], axis=0).T


def merge_pair(halves, chips):
    cores, height, _ = halves.shape
    rows = height // (chips + 1)

    def body(x_ref, out_ref):
        logs = []
        for c in range(cores):
            tail = x_ref[c, chips * rows :, :].astype(jnp.float32)
            logs.append(tail + pltpu.roll(tail, LANES - chips, 1) + pltpu.roll(tail, LANES - 2 * chips, 1))
        top = logs[0]
        for one in logs[1:]:
            top = jnp.maximum(top, one)
        scale = [jnp.exp(one - top) for one in logs]
        norm = sum(scale[1:], scale[0])
        weight = [one / norm for one in scale]
        whole = square(top + jnp.log(norm))[:chips]
        first, second, third = pieces(whole)
        sub = iota((8, LANES), 0)
        for d in range(chips):
            mixed = sum(
                weight[c][:, d : d + 1] * x_ref[c, d * rows : (d + 1) * rows, :].astype(jnp.float32) for c in range(cores)
            )
            out_ref[d, :rows, :] = mixed.astype(jnp.bfloat16)
            tail = jnp.where(sub == 0, first[d : d + 1], jnp.where(sub == 1, second[d : d + 1], third[d : d + 1]))
            out_ref[d, rows:, :] = tail.astype(jnp.bfloat16)

    vmem = pl.BlockSpec(memory_space=pltpu.VMEM)
    return pl.pallas_call(
        body,
        name="merge_pair",
        out_shape=jax.ShapeDtypeStruct((chips, rows + 8, LANES), jnp.bfloat16),
        in_specs=[vmem],
        out_specs=vmem,
        compiler_params=limit(4096),
    )(halves)


def finish(got, requests):
    chips, height, _ = got.shape
    rows = height - 8
    heads = rows // requests

    def body(x_ref, att_ref, log_ref):
        logs = []
        for s in range(chips):
            tail = x_ref[s, rows:, :].astype(jnp.float32)
            logs.append(tail[0:1] + tail[1:2] + tail[2:3])
        logs = jnp.concatenate(logs, axis=0)
        top = jnp.max(logs, axis=0, keepdims=True)
        scale = jnp.exp(logs - top)
        norm = jnp.sum(scale, axis=0, keepdims=True)
        log_norm = jnp.broadcast_to(top + jnp.log(norm), (requests, LANES))
        weight = square(scale / norm)[:rows]
        merged = sum(weight[:, s : s + 1] * x_ref[s, :rows, :].astype(jnp.float32) for s in range(chips))
        att_ref[...] = merged.reshape(requests, heads, LANES).astype(jnp.bfloat16)
        sub = iota((requests, LANES), 0)
        spread = log_norm
        for r in range(1, requests):
            spread = jnp.where(sub == r, pltpu.roll(log_norm, LANES - r * heads, 1), spread)
        log_ref[...] = spread[:, :heads]

    vmem = pl.BlockSpec(memory_space=pltpu.VMEM)
    return pl.pallas_call(
        body,
        name="finish",
        out_shape=(
            jax.ShapeDtypeStruct((requests, heads, LANES), jnp.bfloat16),
            jax.ShapeDtypeStruct((requests, heads), jnp.float32),
        ),
        in_specs=[vmem],
        out_specs=(vmem, vmem),
        compiler_params=limit(4096),
    )(got)


def local(queries, kv_cache, keep, lengths, placement, positions):
    chips, cores = lax.axis_size("dp"), lax.axis_size("sub")
    requests, q_heads, head_dim = queries.shape
    pool_dev, kv_heads, _, block_len, _ = kv_cache.shape
    assert kv_heads == 1
    message = pack(queries, positions, keep, lengths, placement, chips, cores, pool_dev, block_len)
    asked = lax.all_to_all(message, "dp", 0, 0, tiled=True)
    asked = lax.all_gather(asked, "sub")
    partials = attend(kv_cache.reshape(pool_dev, 2, block_len, head_dim), asked, requests)
    halves = lax.all_to_all(partials, "sub", 0, 0, tiled=True)
    answer = lax.all_to_all(merge_pair(halves, chips), "dp", 0, 0, tiled=True)
    return finish(answer, requests)


def solution(mesh):
    in_specs = (
        P(("groups", "dp", "sub"), "head", None),
        P(("groups", "dp", "sub"), "head", None, None, None),
        P(("groups", "dp", "sub"), None),
        P(("groups", "dp", "sub")),
        P(("groups", "dp", "sub"), None),
        P(("groups", "dp", "sub")),
    )
    out_specs = (P(("groups", "dp", "sub"), "head", None), P(("groups", "dp", "sub"), "head"))
    return jax.shard_map(local, mesh=mesh, in_specs=in_specs, out_specs=out_specs, check_vma=False)
```

```python
import jax
import jax.numpy as jnp
import numpy as np
from jax import lax
from jax.experimental import pallas as pl
from jax.experimental.pallas import tpu as pltpu
from jax.sharding import PartitionSpec as P

LANES = 128
LOW = -1e30
LOG2E = 1.4426950408889634
NEAR = 2
UNROLL = True
PACK_LIMIT = 60 * 1024
ATTEND_LIMIT = 52000


def iota(shape, dim):
    return lax.broadcasted_iota(jnp.int32, shape, dim)


def bits(n):
    assert n & (n - 1) == 0
    return n.bit_length() - 1


def frequencies(head_dim, rows):
    half = head_dim // 2
    inverse = 1000000.0 ** (-(2.0 * np.arange(half)) / head_dim)
    return jnp.asarray(np.tile(inverse, (rows, head_dim // half)), jnp.float32)


def limit(kib):
    return pltpu.CompilerParams(vmem_limit_bytes=kib << 10)


def pack(queries, positions, keep, lengths, placement, chips, near, cores, pool_dev, block_len):
    requests, heads, head_dim = queries.shape
    kept, blocks = keep.shape[1], placement.shape[1]
    owners = chips * cores
    spread = requests * blocks // owners
    rows = requests * heads
    parts = requests * blocks // LANES
    per = requests // parts
    assert per * blocks == LANES and 4 * cores * spread == LANES and head_dim == LANES
    pool_bits, owner_bits, len_bits, req_bits = bits(pool_dev), bits(cores), bits(block_len), bits(requests)

    def body(lengths_ref, positions_ref, q_ref, freq_ref, keep_ref, place_ref, out_ref):
        place = place_ref[...]
        kept_ids = keep_ref[...]
        req = iota((requests, blocks), 0)
        lane = iota((requests, blocks), 1)
        length = jnp.zeros((requests, blocks), jnp.int32)
        for r in range(requests):
            length = jnp.where(req == r, lengths_ref[r], length)
        count = jnp.zeros((requests, blocks), jnp.int32)
        for s in range(kept):
            count = jnp.where(kept_ids[:, s : s + 1] == lane, jnp.clip(length - s * block_len, 0, block_len), count)
        owner = place >> pool_bits
        owner = (owner & (cores - 1)) * chips + (owner >> owner_bits)
        word = (place & (pool_dev - 1)) | (req << pool_bits) | (count << (pool_bits + req_bits))
        owner = jnp.concatenate([owner[p * parts : (p + 1) * parts] for p in range(per)], axis=1)
        word = jnp.concatenate([word[p * parts : (p + 1) * parts] for p in range(per)], axis=1).astype(jnp.float32)
        mine = iota((owners, LANES), 0)
        hits = [owner[j : j + 1] == mine for j in range(parts)]
        ones = jnp.concatenate([jnp.where(h, 1.0, 0.0) for h in hits], axis=0).astype(jnp.bfloat16)
        before = jnp.where(iota((LANES, LANES), 0) < iota((LANES, LANES), 1), 1.0, 0.0).astype(jnp.bfloat16)
        within = jnp.dot(ones, before, preferred_element_type=jnp.float32)
        totals = jnp.dot(ones, jnp.ones((LANES, LANES), jnp.bfloat16), preferred_element_type=jnp.float32)
        ranks, start = [], jnp.zeros((owners, LANES), jnp.float32)
        for j in range(parts):
            ranks.append(jnp.where(hits[j], within[j * owners : (j + 1) * owners] + start, -1.0))
            start = start + totals[j * owners : (j + 1) * owners]
        col = iota((owners, LANES), 1)
        table = jnp.zeros((owners, LANES), jnp.float32)
        for k in range(spread):
            found = jnp.zeros((owners, LANES), jnp.float32)
            for j in range(parts):
                found = jnp.where(ranks[j] == k, word[j : j + 1], found)
            table = jnp.where((col & (spread - 1)) == k, jnp.sum(found, axis=1, keepdims=True), table)
        table = table.astype(jnp.int32)
        lane = iota((chips, LANES), 1)
        slots = table[:chips]
        for c in range(1, cores):
            slots = jnp.where(((lane >> bits(spread)) & (cores - 1)) == c, table[c * chips : (c + 1) * chips], slots)
        field = lane >> bits(spread * cores)
        low_bits = bits(block_len)
        row_hi = (slots & (pool_dev - 1)) >> low_bits
        row_lo = slots & (block_len - 1)
        of_req = (slots >> pool_bits) & (requests - 1)
        live = slots >> (pool_bits + req_bits)
        meta = jnp.where(field == 0, row_hi, jnp.where(field == 1, row_lo, jnp.where(field == 2, of_req, live)))
        meta = meta.astype(jnp.float32)
        row = iota((requests, head_dim), 0)
        position = jnp.zeros((requests, head_dim), jnp.int32)
        for r in range(requests):
            position = jnp.where(row == r, positions_ref[r], position)
        angle = position.astype(jnp.float32) * freq_ref[...]
        cosine, sine = jnp.cos(angle), jnp.sin(angle)
        sine = jnp.where(iota((requests, head_dim), 1) < head_dim // 2, -sine, sine)
        turned = []
        for r in range(requests):
            x = q_ref[r].astype(jnp.float32)
            turned.append(x * cosine[r : r + 1] + pltpu.roll(x, head_dim // 2, 1) * sine[r : r + 1])
        turned = jnp.concatenate(turned, axis=0).astype(jnp.bfloat16)
        sub = iota((8, LANES), 0)
        for d in range(chips // near):
            out_ref[d, :rows, :] = turned
            tail = jnp.zeros((8, LANES), jnp.float32)
            for p in range(near):
                tail = jnp.where(sub == p, meta[d * near + p : d * near + p + 1], tail)
            out_ref[d, rows:, :] = tail.astype(jnp.bfloat16)

    vmem = pl.BlockSpec(memory_space=pltpu.VMEM)
    return pl.pallas_call(
        body,
        name="pack",
        out_shape=jax.ShapeDtypeStruct((chips // near, rows + 8, LANES), jnp.bfloat16),
        in_specs=[pl.BlockSpec(memory_space=pltpu.SMEM)] * 2 + [vmem] * 4,
        out_specs=vmem,
        compiler_params=limit(PACK_LIMIT),
    )(lengths, positions, queries, frequencies(head_dim, requests), keep, placement)


def pieces(x):
    first = x.astype(jnp.bfloat16).astype(jnp.float32)
    rest = x - first
    second = rest.astype(jnp.bfloat16).astype(jnp.float32)
    return first, second, rest - second


def attend(kv, got, requests):
    cores, near, far, height, _ = got.shape
    pool_dev, _, block_len, _ = kv.shape
    chips = near * far
    rows = height - 8
    heads = rows // requests
    sources = cores * chips
    spread = LANES // (4 * cores)
    tokens = spread * block_len
    factor = LANES ** (-0.5) * LOG2E
    assert cores == 2

    def body(kv_ref, got_ref, send_ref, keep_ref, k_ref, v_ref, ids_ref, live_ref, weight_ref, rows_ref, sems):
        k_copy = pltpu.make_async_copy(kv_ref.at[:, 0], k_ref, sems.at[0])
        v_copy = pltpu.make_async_copy(kv_ref.at[:, 1], v_ref, sems.at[1])
        k_copy.start()
        me = lax.axis_index("sub")
        at = me * spread
        tails = jnp.concatenate([got_ref[s // chips, s % chips, rows:, :] for s in range(sources)], axis=0)
        mine_row = iota((sources, 8 * sources), 0) * 8 + lax.axis_index("dp") % near
        select = jnp.where(iota((sources, 8 * sources), 1) == mine_row, 1.0, 0.0).astype(jnp.bfloat16)
        meta = jnp.dot(select, tails, preferred_element_type=jnp.float32).astype(jnp.bfloat16)
        wide = cores * spread
        src, dst = iota((LANES, LANES), 0), iota((LANES, LANES), 1)
        inside = dst < spread
        pick = jnp.where(inside & (src == at + dst), float(block_len), 0.0) + jnp.where(inside & (src == wide + at + dst), 1.0, 0.0)
        ids = jnp.dot(meta, pick.astype(jnp.bfloat16), preferred_element_type=jnp.float32)
        ids_ref[...] = ids.astype(jnp.int32)
        copy = pltpu.make_async_copy(ids_ref, rows_ref, sems.at[2])
        copy.start()
        src, dst = iota((LANES, tokens), 0), iota((LANES, tokens), 1) >> bits(block_len)
        pick_req = jnp.where(src == 2 * wide + at + dst, 1.0, 0.0).astype(jnp.bfloat16)
        pick_live = jnp.where(src == 3 * wide + at + dst, 1.0, 0.0).astype(jnp.bfloat16)
        of_req = jnp.dot(meta, pick_req, preferred_element_type=jnp.float32)
        count = jnp.dot(meta, pick_live, preferred_element_type=jnp.float32)
        step = (iota((sources, tokens), 1) & (block_len - 1)).astype(jnp.float32)
        live_ref[...] = jnp.where(step < count, of_req, -1.0)
        request = (iota((rows, tokens), 0) >> bits(heads)).astype(jnp.float32)
        lane = iota((rows, LANES), 1)
        fill = jnp.ones((tokens, LANES), jnp.bfloat16)
        low = jnp.full((rows, LANES), LOW, jnp.float32)
        copy.wait()
        v_copy.start()
        k_copy.wait()

        def held(ref, s):
            return jnp.concatenate([ref[rows_ref[s, k]] for k in range(spread)], axis=0)

        def chip(i):
            return (i & (far - 1)) * near + (i >> bits(far))

        whose = (1 - me, me)
        peaks = []
        for c in whose:

            def look(i, peak_of, c=c):
                s = c * chips + i
                score = (
                    lax.dot_general(
                        got_ref[c, i, :rows, :], held(k_ref, s), (((1,), (1,)), ((), ())), preferred_element_type=jnp.float32
                    )
                    * factor
                )
                mine = live_ref[pl.ds(s, 1), :] == request
                score = jnp.where(mine, score, LOW)
                peak = jnp.max(score, axis=1, keepdims=True)
                weight_ref[s] = jnp.where(mine, jnp.exp2(score - peak), 0.0).astype(jnp.bfloat16)
                return jnp.where(lane == chip(i), peak, peak_of)

            peaks.append(lax.fori_loop(0, chips, look, low, unroll=UNROLL))
        v_copy.wait()
        for c, peak_of, out_ref in zip(whose, peaks, (send_ref, keep_ref)):

            def add(i, total_of, c=c, out_ref=out_ref):
                s = c * chips + i
                vs = jnp.concatenate([held(v_ref, s), fill], axis=1)
                both = jnp.dot(weight_ref[s], vs, preferred_element_type=jnp.float32)
                total = both[:, LANES:]
                safe = jnp.where(total > 0.0, total, 1.0)
                start = pl.multiple_of(chip(i) * rows, rows)
                out_ref[pl.ds(start, rows), :] = (both[:, :LANES] / safe).astype(jnp.bfloat16)
                return jnp.where(lane == chip(i), total, total_of)

            total = lax.fori_loop(0, chips, add, jnp.zeros((rows, LANES), jnp.float32), unroll=UNROLL)
            some = total > 0.0
            logs = peak_of * (1.0 / LOG2E) + jnp.log(jnp.where(some, total, 1.0))
            first, second, third = pieces(jnp.where(some, logs, LOW))
            second, third = pltpu.roll(second, chips, 1), pltpu.roll(third, 2 * chips, 1)
            out_ref[chips * rows :, :] = jnp.where(
                lane < chips, first, jnp.where(lane < 2 * chips, second, third)
            ).astype(jnp.bfloat16)

    vmem = pl.BlockSpec(memory_space=pltpu.VMEM)
    half = jax.ShapeDtypeStruct((chips * rows + rows, LANES), jnp.bfloat16)
    return pl.pallas_call(
        body,
        name="attend",
        out_shape=(half, half),
        in_specs=[pl.BlockSpec(memory_space=pltpu.HBM), vmem],
        out_specs=(vmem, vmem),
        compiler_params=limit(ATTEND_LIMIT),
        scratch_shapes=[
            pltpu.VMEM((pool_dev, block_len, LANES), jnp.bfloat16),
            pltpu.VMEM((pool_dev, block_len, LANES), jnp.bfloat16),
            pltpu.VMEM((sources, LANES), jnp.int32),
            pltpu.VMEM((sources, tokens), jnp.float32),
            pltpu.VMEM((sources, rows, tokens), jnp.bfloat16),
            pltpu.SMEM((sources, LANES), jnp.int32),
            pltpu.SemaphoreType.DMA((3,)),
        ],
    )(kv, got.reshape(cores, chips, height, LANES))


def square(x):
    return jnp.concatenate([x, jnp.zeros((LANES - x.shape[0], LANES), x.dtype)], axis=0).T


def merge_pair(halves, chips):
    cores = len(halves)
    rows = halves[0].shape[0] // (chips + 1)

    def body(*refs):
        x_refs, out_ref = refs[:cores], refs[cores]
        logs = []
        for c in range(cores):
            tail = x_refs[c][chips * rows :, :].astype(jnp.float32)
            logs.append(tail + pltpu.roll(tail, LANES - chips, 1) + pltpu.roll(tail, LANES - 2 * chips, 1))
        top = logs[0]
        for one in logs[1:]:
            top = jnp.maximum(top, one)
        scale = [jnp.exp(one - top) for one in logs]
        norm = sum(scale[1:], scale[0])
        weight = [one / norm for one in scale]
        whole = square(top + jnp.log(norm))[:chips]
        first, second, third = pieces(whole)
        sub = iota((8, LANES), 0)
        for d in range(chips):
            mixed = sum(
                weight[c][:, d : d + 1] * x_refs[c][d * rows : (d + 1) * rows, :].astype(jnp.float32) for c in range(cores)
            )
            out_ref[d, :rows, :] = mixed.astype(jnp.bfloat16)
            tail = jnp.where(sub == 0, first[d : d + 1], jnp.where(sub == 1, second[d : d + 1], third[d : d + 1]))
            out_ref[d, rows:, :] = tail.astype(jnp.bfloat16)

    vmem = pl.BlockSpec(memory_space=pltpu.VMEM)
    return pl.pallas_call(
        body,
        name="merge_pair",
        out_shape=jax.ShapeDtypeStruct((chips, rows + 8, LANES), jnp.bfloat16),
        in_specs=[vmem] * cores,
        out_specs=vmem,
        compiler_params=limit(4096),
    )(*halves)


def finish(got, requests):
    chips, height, _ = got.shape
    rows = height - 8
    heads = rows // requests

    def body(x_ref, att_ref, log_ref):
        logs = []
        for s in range(chips):
            tail = x_ref[s, rows:, :].astype(jnp.float32)
            logs.append(tail[0:1] + tail[1:2] + tail[2:3])
        logs = jnp.concatenate(logs, axis=0)
        top = jnp.max(logs, axis=0, keepdims=True)
        scale = jnp.exp(logs - top)
        norm = jnp.sum(scale, axis=0, keepdims=True)
        log_norm = jnp.broadcast_to(top + jnp.log(norm), (requests, LANES))
        weight = square(scale / norm)[:rows]
        merged = sum(weight[:, s : s + 1] * x_ref[s, :rows, :].astype(jnp.float32) for s in range(chips))
        att_ref[...] = merged.reshape(requests, heads, LANES).astype(jnp.bfloat16)
        sub = iota((requests, LANES), 0)
        spread = log_norm
        for r in range(1, requests):
            spread = jnp.where(sub == r, pltpu.roll(log_norm, LANES - r * heads, 1), spread)
        log_ref[...] = spread[:, :heads]

    vmem = pl.BlockSpec(memory_space=pltpu.VMEM)
    return pl.pallas_call(
        body,
        name="finish",
        out_shape=(
            jax.ShapeDtypeStruct((requests, heads, LANES), jnp.bfloat16),
            jax.ShapeDtypeStruct((requests, heads), jnp.float32),
        ),
        in_specs=[vmem],
        out_specs=(vmem, vmem),
        compiler_params=limit(4096),
    )(got)


def local(queries, kv_cache, keep, lengths, placement, positions):
    chips, cores = lax.axis_size("dp"), lax.axis_size("sub")
    requests, q_heads, head_dim = queries.shape
    pool_dev, kv_heads, _, block_len, _ = kv_cache.shape
    assert kv_heads == 1
    near, far = NEAR, chips // NEAR
    message = pack(queries, positions, keep, lengths, placement, chips, near, cores, pool_dev, block_len)
    apart = [[j * near + p for j in range(far)] for p in range(near)]
    beside = [[j * near + p for p in range(near)] for j in range(far)]
    asked = lax.all_to_all(message, "dp", 0, 0, tiled=True, axis_index_groups=apart)
    asked = lax.all_gather(asked, "dp", axis_index_groups=beside)
    asked = lax.all_gather(asked, "sub")
    send, own = attend(kv_cache.reshape(pool_dev, 2, block_len, head_dim), asked, requests)
    other = lax.ppermute(send, "sub", [(c, (c + 1) % cores) for c in range(cores)])
    answer = lax.all_to_all(merge_pair((own, other), chips), "dp", 0, 0, tiled=True)
    return finish(answer, requests)


def solution(mesh):
    in_specs = (
        P(("groups", "dp", "sub"), "head", None),
        P(("groups", "dp", "sub"), "head", None, None, None),
        P(("groups", "dp", "sub"), None),
        P(("groups", "dp", "sub")),
        P(("groups", "dp", "sub"), None),
        P(("groups", "dp", "sub")),
    )
    out_specs = (P(("groups", "dp", "sub"), "head", None), P(("groups", "dp", "sub"), "head"))
    return jax.shard_map(local, mesh=mesh, in_specs=in_specs, out_specs=out_specs, check_vma=False)
```

```python
import jax
import jax.numpy as jnp
import numpy as np
from jax import lax
from jax.experimental import pallas as pl
from jax.experimental.pallas import tpu as pltpu
from jax.sharding import PartitionSpec as P

LANES = 128
LOW = -1e30
LOG2E = 1.4426950408889634
NEAR = 2
CORES = 2
PACK_LIMIT = 60 * 1024
ATTEND_LIMIT = 52000


def iota(shape, dim):
    return lax.broadcasted_iota(jnp.int32, shape, dim)


def bits(n):
    assert n & (n - 1) == 0
    return n.bit_length() - 1


def frequencies(head_dim, rows):
    half = head_dim // 2
    inverse = 1000000.0 ** (-(2.0 * np.arange(half)) / head_dim)
    return jnp.asarray(np.tile(inverse, (rows, head_dim // half)), jnp.float32)


def limit(kib):
    return pltpu.CompilerParams(vmem_limit_bytes=kib << 10)


def pack(queries, positions, keep, lengths, placement, chips, near, cores, pool_dev, block_len):
    requests, heads, head_dim = queries.shape
    kept, blocks = keep.shape[1], placement.shape[1]
    owners = chips * cores
    spread = requests * blocks // owners
    rows = requests * heads
    parts = requests * blocks // LANES
    per = requests // parts
    assert per * blocks == LANES and 4 * cores * spread == LANES and head_dim == LANES
    pool_bits, owner_bits, len_bits, req_bits = bits(pool_dev), bits(cores), bits(block_len), bits(requests)

    def body(lengths_ref, positions_ref, q_ref, freq_ref, keep_ref, place_ref, out_ref):
        place = place_ref[...]
        kept_ids = keep_ref[...]
        req = iota((requests, blocks), 0)
        lane = iota((requests, blocks), 1)
        length = jnp.zeros((requests, blocks), jnp.int32)
        for r in range(requests):
            length = jnp.where(req == r, lengths_ref[r], length)
        count = jnp.zeros((requests, blocks), jnp.int32)
        for s in range(kept):
            count = jnp.where(kept_ids[:, s : s + 1] == lane, jnp.clip(length - s * block_len, 0, block_len), count)
        owner = place >> pool_bits
        owner = (owner & (cores - 1)) * chips + (owner >> owner_bits)
        word = (place & (pool_dev - 1)) | (req << pool_bits) | (count << (pool_bits + req_bits))
        owner = jnp.concatenate([owner[p * parts : (p + 1) * parts] for p in range(per)], axis=1)
        word = jnp.concatenate([word[p * parts : (p + 1) * parts] for p in range(per)], axis=1).astype(jnp.float32)
        mine = iota((owners, LANES), 0)
        hits = [owner[j : j + 1] == mine for j in range(parts)]
        ones = jnp.concatenate([jnp.where(h, 1.0, 0.0) for h in hits], axis=0).astype(jnp.bfloat16)
        before = jnp.where(iota((LANES, LANES), 0) < iota((LANES, LANES), 1), 1.0, 0.0).astype(jnp.bfloat16)
        within = jnp.dot(ones, before, preferred_element_type=jnp.float32)
        totals = jnp.dot(ones, jnp.ones((LANES, LANES), jnp.bfloat16), preferred_element_type=jnp.float32)
        ranks, start = [], jnp.zeros((owners, LANES), jnp.float32)
        for j in range(parts):
            ranks.append(jnp.where(hits[j], within[j * owners : (j + 1) * owners] + start, -1.0))
            start = start + totals[j * owners : (j + 1) * owners]
        col = iota((owners, LANES), 1)
        table = jnp.zeros((owners, LANES), jnp.float32)
        for k in range(spread):
            found = jnp.zeros((owners, LANES), jnp.float32)
            for j in range(parts):
                found = jnp.where(ranks[j] == k, word[j : j + 1], found)
            table = jnp.where((col & (spread - 1)) == k, jnp.sum(found, axis=1, keepdims=True), table)
        table = table.astype(jnp.int32)
        lane = iota((chips, LANES), 1)
        slots = table[:chips]
        for c in range(1, cores):
            slots = jnp.where(((lane >> bits(spread)) & (cores - 1)) == c, table[c * chips : (c + 1) * chips], slots)
        field = lane >> bits(spread * cores)
        low_bits = bits(block_len)
        row_hi = (slots & (pool_dev - 1)) >> low_bits
        row_lo = slots & (block_len - 1)
        of_req = (slots >> pool_bits) & (requests - 1)
        live = slots >> (pool_bits + req_bits)
        meta = jnp.where(field == 0, row_hi, jnp.where(field == 1, row_lo, jnp.where(field == 2, of_req, live)))
        meta = meta.astype(jnp.float32)
        row = iota((requests, head_dim), 0)
        position = jnp.zeros((requests, head_dim), jnp.int32)
        for r in range(requests):
            position = jnp.where(row == r, positions_ref[r], position)
        angle = position.astype(jnp.float32) * freq_ref[...]
        cosine, sine = jnp.cos(angle), jnp.sin(angle)
        sine = jnp.where(iota((requests, head_dim), 1) < head_dim // 2, -sine, sine)
        turned = []
        for r in range(requests):
            x = q_ref[r].astype(jnp.float32)
            turned.append(x * cosine[r : r + 1] + pltpu.roll(x, head_dim // 2, 1) * sine[r : r + 1])
        turned = jnp.concatenate(turned, axis=0).astype(jnp.bfloat16)
        sub = iota((8, LANES), 0)
        for d in range(chips // near):
            out_ref[d, :rows, :] = turned
            tail = jnp.zeros((8, LANES), jnp.float32)
            for p in range(near):
                tail = jnp.where(sub == p, meta[d * near + p : d * near + p + 1], tail)
            out_ref[d, rows:, :] = tail.astype(jnp.bfloat16)

    vmem = pl.BlockSpec(memory_space=pltpu.VMEM)
    return pl.pallas_call(
        body,
        name="pack",
        out_shape=jax.ShapeDtypeStruct((chips // near, rows + 8, LANES), jnp.bfloat16),
        in_specs=[pl.BlockSpec(memory_space=pltpu.SMEM)] * 2 + [vmem] * 4,
        out_specs=vmem,
        compiler_params=limit(PACK_LIMIT),
    )(lengths, positions, queries, frequencies(head_dim, requests), keep, placement)


def pieces(x):
    first = x.astype(jnp.bfloat16).astype(jnp.float32)
    rest = x - first
    second = rest.astype(jnp.bfloat16).astype(jnp.float32)
    return first, second, rest - second


def abreast(x, width):
    lane = iota(x.shape, 1)
    first, second, third = pieces(x)
    second, third = pltpu.roll(second, width, 1), pltpu.roll(third, 2 * width, 1)
    return jnp.where(lane < width, first, jnp.where(lane < 2 * width, second, third)).astype(jnp.bfloat16)


def together(x, width):
    x = x.astype(jnp.float32)
    return x + pltpu.roll(x, LANES - width, 1) + pltpu.roll(x, LANES - 2 * width, 1)


def attend(kv, got, requests):
    members, far, height, _ = got.shape
    near, cores = members // CORES, CORES
    pool_dev, _, block_len, _ = kv.shape
    chips = near * far
    rows = height - 8
    heads = rows // requests
    sources = cores * chips
    spread = LANES // (4 * cores)
    tokens = spread * block_len
    factor = LANES ** (-0.5) * LOG2E

    def body(kv_ref, got_ref, send_ref, keep_ref, k_ref, v_ref, ids_ref, live_ref, weight_ref, rows_ref, sems):
        k_copy = pltpu.make_async_copy(kv_ref.at[:, 0], k_ref, sems.at[0])
        v_copy = pltpu.make_async_copy(kv_ref.at[:, 1], v_ref, sems.at[1])
        k_copy.start()
        me = lax.axis_index("sub")
        at = me * spread
        tails = jnp.concatenate([got_ref[s, rows:, :] for s in range(sources)], axis=0)
        mine_row = iota((sources, 8 * sources), 0) * 8 + lax.axis_index("dp") % near
        select = jnp.where(iota((sources, 8 * sources), 1) == mine_row, 1.0, 0.0).astype(jnp.bfloat16)
        meta = jnp.dot(select, tails, preferred_element_type=jnp.float32).astype(jnp.bfloat16)
        wide = cores * spread
        src, dst = iota((LANES, LANES), 0), iota((LANES, LANES), 1)
        inside = dst < spread
        pick = jnp.where(inside & (src == at + dst), float(block_len), 0.0) + jnp.where(inside & (src == wide + at + dst), 1.0, 0.0)
        ids = jnp.dot(meta, pick.astype(jnp.bfloat16), preferred_element_type=jnp.float32)
        ids_ref[...] = ids.astype(jnp.int32)
        copy = pltpu.make_async_copy(ids_ref, rows_ref, sems.at[2])
        copy.start()
        src, dst = iota((LANES, tokens), 0), iota((LANES, tokens), 1) >> bits(block_len)
        pick_req = jnp.where(src == 2 * wide + at + dst, 1.0, 0.0).astype(jnp.bfloat16)
        pick_live = jnp.where(src == 3 * wide + at + dst, 1.0, 0.0).astype(jnp.bfloat16)
        of_req = jnp.dot(meta, pick_req, preferred_element_type=jnp.float32)
        count = jnp.dot(meta, pick_live, preferred_element_type=jnp.float32)
        step = (iota((sources, tokens), 1) & (block_len - 1)).astype(jnp.float32)
        live_ref[...] = jnp.where(step < count, of_req, -1.0)
        request = (iota((rows, tokens), 0) >> bits(heads)).astype(jnp.float32)
        lane = iota((rows, LANES), 1)
        fill = jnp.ones((tokens, LANES), jnp.bfloat16)
        low = jnp.full((rows, LANES), LOW, jnp.float32)
        copy.wait()
        v_copy.start()
        k_copy.wait()

        def held(ref, s):
            return jnp.concatenate([ref[rows_ref[s, k]] for k in range(spread)], axis=0)

        this = lax.axis_index("dp") % near

        def source(c, t):
            return (((this + 1 + t // far) % near) * cores + c) * far + t % far

        whose = (1 - me, me)
        peaks = []
        for c in whose:

            peak_of = low
            for t in range(chips):
                s = source(c, t)
                score = (
                    lax.dot_general(
                        got_ref[s, :rows, :], held(k_ref, s), (((1,), (1,)), ((), ())), preferred_element_type=jnp.float32
                    )
                    * factor
                )
                mine = live_ref[pl.ds(s, 1), :] == request
                score = jnp.where(mine, score, LOW)
                peak = jnp.max(score, axis=1, keepdims=True)
                weight_ref[s] = jnp.where(mine, jnp.exp2(score - peak), 0.0).astype(jnp.bfloat16)
                peak_of = jnp.where(lane == t, peak, peak_of)
            peaks.append(peak_of)
        v_copy.wait()
        for c, peak_of, out_ref in zip(whose, peaks, (send_ref, keep_ref)):
            total_of = jnp.zeros((rows, LANES), jnp.float32)
            for t in range(chips):
                s = source(c, t)
                vs = jnp.concatenate([held(v_ref, s), fill], axis=1)
                both = jnp.dot(weight_ref[s], vs, preferred_element_type=jnp.float32)
                total = both[:, LANES:]
                safe = jnp.where(total > 0.0, total, 1.0)
                out_ref[t * rows : (t + 1) * rows, :] = (both[:, :LANES] / safe).astype(out_ref.dtype)
                total_of = jnp.where(lane == t, total, total_of)
            some = total_of > 0.0
            logs = peak_of * (1.0 / LOG2E) + jnp.log(jnp.where(some, total_of, 1.0))
            logs = jnp.where(some, logs, LOW)
            out_ref[chips * rows :, :] = logs if out_ref is keep_ref else abreast(logs, chips)

    vmem = pl.BlockSpec(memory_space=pltpu.VMEM)
    half = (chips * rows + rows, LANES)
    return pl.pallas_call(
        body,
        name="attend",
        out_shape=(jax.ShapeDtypeStruct(half, jnp.bfloat16), jax.ShapeDtypeStruct(half, jnp.float32)),
        in_specs=[pl.BlockSpec(memory_space=pltpu.HBM), vmem],
        out_specs=(vmem, vmem),
        compiler_params=limit(ATTEND_LIMIT),
        scratch_shapes=[
            pltpu.VMEM((pool_dev, block_len, LANES), jnp.bfloat16),
            pltpu.VMEM((pool_dev, block_len, LANES), jnp.bfloat16),
            pltpu.VMEM((sources, LANES), jnp.int32),
            pltpu.VMEM((sources, tokens), jnp.float32),
            pltpu.VMEM((sources, rows, tokens), jnp.bfloat16),
            pltpu.SMEM((sources, LANES), jnp.int32),
            pltpu.SemaphoreType.DMA((3,)),
        ],
    )(kv, got.reshape(sources, height, LANES))


def square(x):
    return jnp.concatenate([x, jnp.zeros((LANES - x.shape[0], LANES), x.dtype)], axis=0).T


def merge(keep, got, axis, width, rows, last):
    near = got.shape[0]
    assert near == 2

    def body(keep_ref, got_ref, *outs):
        partner = near - 1 - lax.axis_index(axis) % near
        mine = keep_ref[width * rows :, :]
        other = together(got_ref[partner, width * rows :, :], width)
        top = jnp.maximum(mine, other)
        mine, other = jnp.exp(mine - top), jnp.exp(other - top)
        norm = mine + other
        mine, other = mine / norm, other / norm
        logs = top + jnp.log(norm)

        def mixed(d):
            own = mine[:, d : d + 1] * keep_ref[d * rows : (d + 1) * rows, :]
            return own + other[:, d : d + 1] * got_ref[partner, d * rows : (d + 1) * rows, :].astype(jnp.float32)

        if not last:
            part = width // 2
            for d in range(part):
                outs[0][d * rows : (d + 1) * rows, :] = mixed(d).astype(jnp.bfloat16)
                outs[1][d * rows : (d + 1) * rows, :] = mixed(part + d)
            outs[0][part * rows :, :] = abreast(logs, part)
            outs[1][part * rows :, :] = pltpu.roll(logs, LANES - part, 1)
            return
        first, second, third = pieces(square(logs)[:width])
        sub = iota((8, LANES), 0)
        for d in range(width):
            outs[0][d, :rows, :] = mixed(d).astype(jnp.bfloat16)
            tail = jnp.where(sub == 0, first[d : d + 1], jnp.where(sub == 1, second[d : d + 1], third[d : d + 1]))
            outs[0][d, rows:, :] = tail.astype(jnp.bfloat16)

    vmem = pl.BlockSpec(memory_space=pltpu.VMEM)
    if last:
        out_shape = (jax.ShapeDtypeStruct((width, rows + 8, LANES), jnp.bfloat16),)
    else:
        half = (width // 2 * rows + rows, LANES)
        out_shape = (jax.ShapeDtypeStruct(half, jnp.bfloat16), jax.ShapeDtypeStruct(half, jnp.float32))
    return pl.pallas_call(
        body,
        name="merge_" + axis,
        out_shape=out_shape,
        in_specs=[vmem, vmem],
        out_specs=(vmem,) * len(out_shape),
        compiler_params=limit(4096),
    )(keep, got)


def finish(got, requests):
    chips, height, _ = got.shape
    rows = height - 8
    heads = rows // requests

    def body(x_ref, att_ref, log_ref):
        logs = []
        for s in range(chips):
            tail = x_ref[s, rows:, :].astype(jnp.float32)
            logs.append(tail[0:1] + tail[1:2] + tail[2:3])
        logs = jnp.concatenate(logs, axis=0)
        top = jnp.max(logs, axis=0, keepdims=True)
        scale = jnp.exp(logs - top)
        norm = jnp.sum(scale, axis=0, keepdims=True)
        log_norm = jnp.broadcast_to(top + jnp.log(norm), (requests, LANES))
        weight = square(scale / norm)[:rows]
        merged = sum(weight[:, s : s + 1] * x_ref[s, :rows, :].astype(jnp.float32) for s in range(chips))
        att_ref[...] = merged.reshape(requests, heads, LANES).astype(jnp.bfloat16)
        sub = iota((requests, LANES), 0)
        spread = log_norm
        for r in range(1, requests):
            spread = jnp.where(sub == r, pltpu.roll(log_norm, LANES - r * heads, 1), spread)
        log_ref[...] = spread[:, :heads]

    vmem = pl.BlockSpec(memory_space=pltpu.VMEM)
    return pl.pallas_call(
        body,
        name="finish",
        out_shape=(
            jax.ShapeDtypeStruct((requests, heads, LANES), jnp.bfloat16),
            jax.ShapeDtypeStruct((requests, heads), jnp.float32),
        ),
        in_specs=[vmem],
        out_specs=(vmem, vmem),
        compiler_params=limit(4096),
    )(got)


def local(queries, kv_cache, keep, lengths, placement, positions):
    chips, cores = lax.axis_size("dp"), lax.axis_size("sub")
    requests, q_heads, head_dim = queries.shape
    pool_dev, kv_heads, _, block_len, _ = kv_cache.shape
    assert kv_heads == 1 and cores == CORES
    near, far = NEAR, chips // NEAR
    message = pack(queries, positions, keep, lengths, placement, chips, near, cores, pool_dev, block_len)
    apart = [[j * near + p for j in range(far)] for p in range(near)]
    beside = [[j * near + p for p in range(near)] for j in range(far)]
    asked = lax.all_to_all(message, "dp", 0, 0, tiled=True, axis_index_groups=apart)
    around = [[j * near * cores + m for m in range(near * cores)] for j in range(far)]
    asked = lax.all_gather(asked, ("dp", "sub"), axis_index_groups=around)
    rows = requests * q_heads
    send, own = attend(kv_cache.reshape(pool_dev, 2, block_len, head_dim), asked, requests)
    send, own = merge(own, lax.all_gather(send, "sub"), "sub", chips, rows, False)
    (answer,) = merge(own, lax.all_gather(send, "dp", axis_index_groups=beside), "dp", far, rows, True)
    answer = lax.all_to_all(answer, "dp", 0, 0, tiled=True, axis_index_groups=apart)
    return finish(answer, requests)


def solution(mesh):
    in_specs = (
        P(("groups", "dp", "sub"), "head", None),
        P(("groups", "dp", "sub"), "head", None, None, None),
        P(("groups", "dp", "sub"), None),
        P(("groups", "dp", "sub")),
        P(("groups", "dp", "sub"), None),
        P(("groups", "dp", "sub")),
    )
    out_specs = (P(("groups", "dp", "sub"), "head", None), P(("groups", "dp", "sub"), "head"))
    return jax.shard_map(local, mesh=mesh, in_specs=in_specs, out_specs=out_specs, check_vma=False)
```

```python
import jax
import jax.numpy as jnp
import numpy as np
from jax import lax
from jax.experimental import pallas as pl
from jax.experimental.pallas import tpu as pltpu
from jax.sharding import PartitionSpec as P

LANES = 128
LOW = -1e30
LOG2E = 1.4426950408889634
NEAR = 2
CORES = 2
PACK_LIMIT = 60 * 1024
ATTEND_LIMIT = 52000


def iota(shape, dim):
    return lax.broadcasted_iota(jnp.int32, shape, dim)


def bits(n):
    assert n & (n - 1) == 0
    return n.bit_length() - 1


def frequencies(head_dim, rows):
    half = head_dim // 2
    inverse = 1000000.0 ** (-(2.0 * np.arange(half)) / head_dim)
    return jnp.asarray(np.tile(inverse, (rows, head_dim // half)), jnp.float32)


def limit(kib):
    return pltpu.CompilerParams(vmem_limit_bytes=kib << 10)


def pack(queries, positions, keep, lengths, placement, chips, near, cores, pool_dev, block_len):
    requests, heads, head_dim = queries.shape
    kept, blocks = keep.shape[1], placement.shape[1]
    owners = chips * cores
    spread = requests * blocks // owners
    rows = requests * heads
    parts = requests * blocks // LANES
    per = requests // parts
    assert per * blocks == LANES and 4 * cores * spread == LANES and head_dim == LANES
    pool_bits, owner_bits, len_bits, req_bits = bits(pool_dev), bits(cores), bits(block_len), bits(requests)

    def body(lengths_ref, positions_ref, q_ref, freq_ref, keep_ref, place_ref, out_ref):
        place = place_ref[...]
        kept_ids = keep_ref[...]
        req = iota((requests, blocks), 0)
        lane = iota((requests, blocks), 1)
        length = jnp.zeros((requests, blocks), jnp.int32)
        for r in range(requests):
            length = jnp.where(req == r, lengths_ref[r], length)
        count = jnp.zeros((requests, blocks), jnp.int32)
        for s in range(kept):
            count = jnp.where(kept_ids[:, s : s + 1] == lane, jnp.clip(length - s * block_len, 0, block_len), count)
        owner = place >> pool_bits
        owner = (owner & (cores - 1)) * chips + (owner >> owner_bits)
        word = (place & (pool_dev - 1)) | (req << pool_bits) | (count << (pool_bits + req_bits))
        owner = jnp.concatenate([owner[p * parts : (p + 1) * parts] for p in range(per)], axis=1)
        word = jnp.concatenate([word[p * parts : (p + 1) * parts] for p in range(per)], axis=1).astype(jnp.float32)
        mine = iota((owners, LANES), 0)
        hits = [owner[j : j + 1] == mine for j in range(parts)]
        ones = jnp.concatenate([jnp.where(h, 1.0, 0.0) for h in hits], axis=0).astype(jnp.bfloat16)
        before = jnp.where(iota((LANES, LANES), 0) < iota((LANES, LANES), 1), 1.0, 0.0).astype(jnp.bfloat16)
        within = jnp.dot(ones, before, preferred_element_type=jnp.float32)
        totals = jnp.dot(ones, jnp.ones((LANES, LANES), jnp.bfloat16), preferred_element_type=jnp.float32)
        ranks, start = [], jnp.zeros((owners, LANES), jnp.float32)
        for j in range(parts):
            ranks.append(jnp.where(hits[j], within[j * owners : (j + 1) * owners] + start, -1.0))
            start = start + totals[j * owners : (j + 1) * owners]
        col = iota((owners, LANES), 1)
        table = jnp.zeros((owners, LANES), jnp.float32)
        for k in range(spread):
            found = jnp.zeros((owners, LANES), jnp.float32)
            for j in range(parts):
                found = jnp.where(ranks[j] == k, word[j : j + 1], found)
            table = jnp.where((col & (spread - 1)) == k, jnp.sum(found, axis=1, keepdims=True), table)
        table = table.astype(jnp.int32)
        lane = iota((chips, LANES), 1)
        slots = table[:chips]
        for c in range(1, cores):
            slots = jnp.where(((lane >> bits(spread)) & (cores - 1)) == c, table[c * chips : (c + 1) * chips], slots)
        field = lane >> bits(spread * cores)
        low_bits = bits(block_len)
        row_hi = (slots & (pool_dev - 1)) >> low_bits
        row_lo = slots & (block_len - 1)
        of_req = (slots >> pool_bits) & (requests - 1)
        live = slots >> (pool_bits + req_bits)
        meta = jnp.where(field == 0, row_hi, jnp.where(field == 1, row_lo, jnp.where(field == 2, of_req, live)))
        meta = meta.astype(jnp.float32)
        row = iota((requests, head_dim), 0)
        position = jnp.zeros((requests, head_dim), jnp.int32)
        for r in range(requests):
            position = jnp.where(row == r, positions_ref[r], position)
        angle = position.astype(jnp.float32) * freq_ref[...]
        cosine, sine = jnp.cos(angle), jnp.sin(angle)
        sine = jnp.where(iota((requests, head_dim), 1) < head_dim // 2, -sine, sine)
        turned = []
        for r in range(requests):
            x = q_ref[r].astype(jnp.float32)
            turned.append(x * cosine[r : r + 1] + pltpu.roll(x, head_dim // 2, 1) * sine[r : r + 1])
        turned = jnp.concatenate(turned, axis=0).astype(jnp.bfloat16)
        sub = iota((8, LANES), 0)
        for d in range(chips // near):
            out_ref[d, :rows, :] = turned
            tail = jnp.zeros((8, LANES), jnp.float32)
            for p in range(near):
                tail = jnp.where(sub == p, meta[d * near + p : d * near + p + 1], tail)
            out_ref[d, rows:, :] = tail.astype(jnp.bfloat16)

    vmem = pl.BlockSpec(memory_space=pltpu.VMEM)
    return pl.pallas_call(
        body,
        name="pack",
        out_shape=jax.ShapeDtypeStruct((chips // near, rows + 8, LANES), jnp.bfloat16),
        in_specs=[pl.BlockSpec(memory_space=pltpu.SMEM)] * 2 + [vmem] * 4,
        out_specs=vmem,
        compiler_params=limit(PACK_LIMIT),
    )(lengths, positions, queries, frequencies(head_dim, requests), keep, placement)


def pieces(x):
    first = x.astype(jnp.bfloat16).astype(jnp.float32)
    rest = x - first
    second = rest.astype(jnp.bfloat16).astype(jnp.float32)
    return first, second, rest - second


def abreast(x, width):
    lane = iota(x.shape, 1)
    first, second, third = pieces(x)
    second, third = pltpu.roll(second, width, 1), pltpu.roll(third, 2 * width, 1)
    return jnp.where(lane < width, first, jnp.where(lane < 2 * width, second, third)).astype(jnp.bfloat16)


def together(x, width):
    x = x.astype(jnp.float32)
    return x + pltpu.roll(x, LANES - width, 1) + pltpu.roll(x, LANES - 2 * width, 1)


def attend(kv, got, requests):
    members, far, height, _ = got.shape
    near, cores = members // CORES, CORES
    pool_dev, _, block_len, _ = kv.shape
    chips = near * far
    rows = height - 8
    heads = rows // requests
    sources = cores * chips
    spread = LANES // (4 * cores)
    tokens = spread * block_len
    factor = LANES ** (-0.5) * LOG2E

    def body(kv_ref, got_ref, send_ref, keep_ref, k_ref, v_ref, ids_ref, live_ref, weight_ref, rows_ref, sems):
        k_copy = pltpu.make_async_copy(kv_ref.at[:, 0], k_ref, sems.at[0])
        v_copy = pltpu.make_async_copy(kv_ref.at[:, 1], v_ref, sems.at[1])
        k_copy.start()
        me = lax.axis_index("sub")
        at = me * spread
        tails = jnp.concatenate([got_ref[s, rows:, :] for s in range(sources)], axis=0)
        mine_row = iota((sources, 8 * sources), 0) * 8 + lax.axis_index("dp") % near
        select = jnp.where(iota((sources, 8 * sources), 1) == mine_row, 1.0, 0.0).astype(jnp.bfloat16)
        meta = jnp.dot(select, tails, preferred_element_type=jnp.float32).astype(jnp.bfloat16)
        wide = cores * spread
        src, dst = iota((LANES, LANES), 0), iota((LANES, LANES), 1)
        inside = dst < spread
        pick = jnp.where(inside & (src == at + dst), float(block_len), 0.0) + jnp.where(inside & (src == wide + at + dst), 1.0, 0.0)
        ids = jnp.dot(meta, pick.astype(jnp.bfloat16), preferred_element_type=jnp.float32)
        ids_ref[...] = ids.astype(jnp.int32)
        copy = pltpu.make_async_copy(ids_ref, rows_ref, sems.at[2])
        copy.start()
        src, dst = iota((LANES, tokens), 0), iota((LANES, tokens), 1) >> bits(block_len)
        pick_req = jnp.where(src == 2 * wide + at + dst, 1.0, 0.0).astype(jnp.bfloat16)
        pick_live = jnp.where(src == 3 * wide + at + dst, 1.0, 0.0).astype(jnp.bfloat16)
        of_req = jnp.dot(meta, pick_req, preferred_element_type=jnp.float32)
        count = jnp.dot(meta, pick_live, preferred_element_type=jnp.float32)
        step = (iota((sources, tokens), 1) & (block_len - 1)).astype(jnp.float32)
        live_ref[...] = jnp.where(step < count, of_req, -1.0)
        request = (iota((rows, tokens), 0) >> bits(heads)).astype(jnp.float32)
        lane = iota((rows, LANES), 1)
        fill = jnp.ones((tokens, LANES), jnp.bfloat16)
        low = jnp.full((rows, LANES), LOW, jnp.float32)
        copy.wait()
        v_copy.start()
        k_copy.wait()

        def held(ref, s):
            return jnp.concatenate([ref[rows_ref[s, k]] for k in range(spread)], axis=0)


        def source(c, t):
            return ((t % near) * cores + c) * far + t // near

        whose = (1 - me, me)
        peaks = []
        for c in whose:

            peak_of = low
            for t in range(chips):
                s = source(c, t)
                score = (
                    lax.dot_general(
                        got_ref[s, :rows, :], held(k_ref, s), (((1,), (1,)), ((), ())), preferred_element_type=jnp.float32
                    )
                    * factor
                )
                mine = live_ref[pl.ds(s, 1), :] == request
                score = jnp.where(mine, score, LOW)
                peak = jnp.max(score, axis=1, keepdims=True)
                weight_ref[s] = jnp.where(mine, jnp.exp2(score - peak), 0.0).astype(jnp.bfloat16)
                peak_of = jnp.where(lane == t, peak, peak_of)
            peaks.append(peak_of)
        v_copy.wait()
        for c, peak_of, out_ref in zip(whose, peaks, (send_ref, keep_ref)):
            total_of = jnp.zeros((rows, LANES), jnp.float32)
            for t in range(chips):
                s = source(c, t)
                vs = jnp.concatenate([held(v_ref, s), fill], axis=1)
                both = jnp.dot(weight_ref[s], vs, preferred_element_type=jnp.float32)
                total = both[:, LANES:]
                safe = jnp.where(total > 0.0, total, 1.0)
                out_ref[t * rows : (t + 1) * rows, :] = (both[:, :LANES] / safe).astype(out_ref.dtype)
                total_of = jnp.where(lane == t, total, total_of)
            some = total_of > 0.0
            logs = peak_of * (1.0 / LOG2E) + jnp.log(jnp.where(some, total_of, 1.0))
            logs = jnp.where(some, logs, LOW)
            out_ref[chips * rows :, :] = logs if out_ref is keep_ref else abreast(logs, chips)

    vmem = pl.BlockSpec(memory_space=pltpu.VMEM)
    half = (chips * rows + rows, LANES)
    return pl.pallas_call(
        body,
        name="attend",
        out_shape=(jax.ShapeDtypeStruct(half, jnp.bfloat16), jax.ShapeDtypeStruct(half, jnp.float32)),
        in_specs=[pl.BlockSpec(memory_space=pltpu.HBM), vmem],
        out_specs=(vmem, vmem),
        compiler_params=limit(ATTEND_LIMIT),
        scratch_shapes=[
            pltpu.VMEM((pool_dev, block_len, LANES), jnp.bfloat16),
            pltpu.VMEM((pool_dev, block_len, LANES), jnp.bfloat16),
            pltpu.VMEM((sources, LANES), jnp.int32),
            pltpu.VMEM((sources, tokens), jnp.float32),
            pltpu.VMEM((sources, rows, tokens), jnp.bfloat16),
            pltpu.SMEM((sources, LANES), jnp.int32),
            pltpu.SemaphoreType.DMA((3,)),
        ],
    )(kv, got.reshape(sources, height, LANES))


def square(x):
    return jnp.concatenate([x, jnp.zeros((LANES - x.shape[0], LANES), x.dtype)], axis=0).T


def merge(keep, got, rows):
    cores = got.shape[0]
    chips = keep.shape[0] // rows - 1
    assert cores == 2

    def body(keep_ref, got_ref, out_ref):
        partner = cores - 1 - lax.axis_index("sub")
        mine = keep_ref[chips * rows :, :]
        other = together(got_ref[partner, chips * rows :, :], chips)
        top = jnp.maximum(mine, other)
        mine, other = jnp.exp(mine - top), jnp.exp(other - top)
        norm = mine + other
        mine, other = mine / norm, other / norm
        first, second, third = pieces(square(top + jnp.log(norm))[:chips])
        sub = iota((8, LANES), 0)
        for d in range(chips):
            at = slice(d * rows, (d + 1) * rows)
            mixed = mine[:, d : d + 1] * keep_ref[at, :] + other[:, d : d + 1] * got_ref[partner, at, :].astype(jnp.float32)
            out_ref[d, :rows, :] = mixed.astype(jnp.bfloat16)
            tail = jnp.where(sub == 0, first[d : d + 1], jnp.where(sub == 1, second[d : d + 1], third[d : d + 1]))
            out_ref[d, rows:, :] = tail.astype(jnp.bfloat16)

    vmem = pl.BlockSpec(memory_space=pltpu.VMEM)
    return pl.pallas_call(
        body,
        name="merge",
        out_shape=jax.ShapeDtypeStruct((chips, rows + 8, LANES), jnp.bfloat16),
        in_specs=[vmem, vmem],
        out_specs=vmem,
        compiler_params=limit(4096),
    )(keep, got)


def finish(got, requests):
    chips, height, _ = got.shape
    rows = height - 8
    heads = rows // requests

    def body(x_ref, att_ref, log_ref):
        logs = []
        for s in range(chips):
            tail = x_ref[s, rows:, :].astype(jnp.float32)
            logs.append(tail[0:1] + tail[1:2] + tail[2:3])
        logs = jnp.concatenate(logs, axis=0)
        top = jnp.max(logs, axis=0, keepdims=True)
        scale = jnp.exp(logs - top)
        norm = jnp.sum(scale, axis=0, keepdims=True)
        log_norm = jnp.broadcast_to(top + jnp.log(norm), (requests, LANES))
        weight = square(scale / norm)[:rows]
        merged = sum(weight[:, s : s + 1] * x_ref[s, :rows, :].astype(jnp.float32) for s in range(chips))
        att_ref[...] = merged.reshape(requests, heads, LANES).astype(jnp.bfloat16)
        sub = iota((requests, LANES), 0)
        spread = log_norm
        for r in range(1, requests):
            spread = jnp.where(sub == r, pltpu.roll(log_norm, LANES - r * heads, 1), spread)
        log_ref[...] = spread[:, :heads]

    vmem = pl.BlockSpec(memory_space=pltpu.VMEM)
    return pl.pallas_call(
        body,
        name="finish",
        out_shape=(
            jax.ShapeDtypeStruct((requests, heads, LANES), jnp.bfloat16),
            jax.ShapeDtypeStruct((requests, heads), jnp.float32),
        ),
        in_specs=[vmem],
        out_specs=(vmem, vmem),
        compiler_params=limit(4096),
    )(got)


def local(queries, kv_cache, keep, lengths, placement, positions):
    chips, cores = lax.axis_size("dp"), lax.axis_size("sub")
    requests, q_heads, head_dim = queries.shape
    pool_dev, kv_heads, _, block_len, _ = kv_cache.shape
    assert kv_heads == 1 and cores == CORES
    near, far = NEAR, chips // NEAR
    message = pack(queries, positions, keep, lengths, placement, chips, near, cores, pool_dev, block_len)
    apart = [[j * near + p for j in range(far)] for p in range(near)]
    asked = lax.all_to_all(message, "dp", 0, 0, tiled=True, axis_index_groups=apart)
    around = [[j * near * cores + m for m in range(near * cores)] for j in range(far)]
    asked = lax.all_gather(asked, ("dp", "sub"), axis_index_groups=around)
    rows = requests * q_heads
    send, own = attend(kv_cache.reshape(pool_dev, 2, block_len, head_dim), asked, requests)
    answer = merge(own, lax.all_gather(send, "sub"), rows)
    answer = lax.all_to_all(answer, "dp", 0, 0, tiled=True)
    return finish(answer, requests)


def solution(mesh):
    in_specs = (
        P(("groups", "dp", "sub"), "head", None),
        P(("groups", "dp", "sub"), "head", None, None, None),
        P(("groups", "dp", "sub"), None),
        P(("groups", "dp", "sub")),
        P(("groups", "dp", "sub"), None),
        P(("groups", "dp", "sub")),
    )
    out_specs = (P(("groups", "dp", "sub"), "head", None), P(("groups", "dp", "sub"), "head"))
    return jax.shard_map(local, mesh=mesh, in_specs=in_specs, out_specs=out_specs, check_vma=False)
```
